32 devices in a mesh: gx: 2 (over y), gy: 4 (over x, core), gz: 4 (over z).
Axes of the slice: x: 2, y: 2, z: 4, core: 2. Of those that a mesh axis runs over, the one named last changes fastest.
Arguments:
- halo_position: float32 [3, 16, 16, 8, 128], P(None, 'gx', 'gy', 'gz'), may hold values from 0 to 1
- halo_velocity: float32 [3, 16, 16, 8, 128], P(None, 'gx', 'gy', 'gz'), may hold values from -1 to 1
- halo_mass: float32 [16, 16, 8, 128], P('gx', 'gy', 'gz'), may hold values from 0.005 to 0.08
- cell_counts: int32 [16, 16, 8], P('gx', 'gy', 'gz'), may hold values from 1 to 128, as said below
Outputs:
- predicted: float32 [3, 16, 16, 8, 128], P(None, 'gx', 'gy', 'gz')
The draws below stay inside these ranges and needn't reach their ends.
Inputs may be any that keep to these rules, and one draw needn't show every extreme that they name: `cell_counts`: slots of a cell from its count on hold no halo.
All inputs are finite; a program needn't handle non-finite values.
Results may differ from the reference program's by a relative error of at most 0.0001.
Values sent between devices are 32-bit elements; how exact they have to be, the bound alone decides.
A program may use at most 64 MiB of HBM per device.

```python
import math
import jax
import jax.numpy as jnp
from jax import lax

CX = 8
CY = 4
CZ = 2
SLOTS = 128
NX = 16
NY = 16
NZ = 8


def draw_cell_counts(key, part):
    key_level, key_fill, key_peak = jax.random.split(key, 3)
    levels = jax.random.randint(key_level, (NX // CX, NY // CY, NZ // CZ), 0, 4)
    factor = jnp.left_shift(jnp.ones_like(levels), levels)
    factor = jnp.repeat(jnp.repeat(jnp.repeat(factor, CX, axis=0), CY, axis=1), CZ, axis=2)
    filled = jax.random.randint(key_fill, (NX, NY, NZ), 0, max(SLOTS // 4, 1))
    counts = jnp.minimum(1 + factor * filled, SLOTS)
    peak_cell = jax.random.randint(key_peak, (), 0, NX * NY * NZ)
    flattened = jnp.where(jnp.arange(NX * NY * NZ) == peak_cell, SLOTS, counts.reshape(-1))
    return flattened.reshape(NX, NY, NZ).astype(jnp.int32)


def steps_of(key, dims, cuts, least, top_value):
    def one(position, blocks):
        heights = jax.random.uniform(jax.random.fold_in(jax.random.fold_in(key, 6), position), (blocks,), jnp.float32, least / len(cuts), top_value / len(cuts))
        return jnp.repeat(jnp.exp(heights), dims[position] // blocks).reshape((-1,) + (1,) * (len(dims) - position - 1))

    loudness = one(*cuts[0])
    for cut in cuts[1:]:
        loudness = loudness * one(*cut)
    return loudness


def scatter_about(rng, extent, width, limit, cuts=(), kind=jnp.bfloat16):
    entries = width * jax.random.normal(rng, extent, jnp.float32)
    if cuts:
        entries = entries * steps_of(rng, extent, cuts, -0.22, 0.18)
    return jnp.clip(entries, -limit, limit).astype(kind)


def setup_inputs(seed: int = 0) -> dict:
    key_of = jax.random.split(jax.random.key(seed), 5)
    halo_position = jnp.clip(1.0 * jax.random.uniform(key_of[0], (3, NX, NY, NZ, SLOTS), jnp.float32) ** steps_of(key_of[0], (3, NX, NY, NZ, SLOTS), ((1, 2), (2, 4), (3, 4)), -0.2, 0.2), 0.0, 1.0)
    halo_velocity = scatter_about(key_of[1], (3, NX, NY, NZ, SLOTS), 0.2, 1.0, ((1, 2), (2, 4), (3, 4)), jnp.float32)
    halo_mass = jnp.clip(jnp.exp(math.log(0.08) - 2.7725887 * jax.random.uniform(key_of[2], (NX, NY, NZ, SLOTS), jnp.float32) ** steps_of(key_of[2], (NX, NY, NZ, SLOTS), ((0, 2), (1, 4), (2, 4)), -0.2, 0.2)), 0.005, 0.08)
    cell_counts = draw_cell_counts(jax.random.fold_in(key_of[4], 71), 0)
    return dict(halo_position=halo_position, halo_velocity=halo_velocity, halo_mass=halo_mass, cell_counts=cell_counts)


soft_sq = 0.01
cut_sq = 0.64

def pull_block(extended, targets):
    depth_x, depth_y, depth_z, slot_count = targets.shape[1:]
    anchor = jnp.int32(0)

    def add_offset(offset_code, running):
        offset_code = offset_code.astype(jnp.int32)
        shift_x = offset_code // 9
        shift_y = offset_code // 3 % 3
        shift_z = offset_code % 3
        sources = lax.dynamic_slice(extended, (anchor, shift_x, shift_y, shift_z, anchor), (4, depth_x, depth_y, depth_z, slot_count))
        delta_x = (sources[0] + (shift_x - 1).astype(jnp.float32))[..., :, None] - targets[0][..., None, :]
        delta_y = (sources[1] + (shift_y - 1).astype(jnp.float32))[..., :, None] - targets[1][..., None, :]
        delta_z = (sources[2] + (shift_z - 1).astype(jnp.float32))[..., :, None] - targets[2][..., None, :]
        dist_sq = delta_x * delta_x + delta_y * delta_y + delta_z * delta_z
        inv_dist = lax.rsqrt(dist_sq + soft_sq)
        tapering = jnp.maximum(1.0 - dist_sq / cut_sq, 0.0)
        weights = sources[3][..., :, None] * (inv_dist * inv_dist * inv_dist) * (tapering * tapering)
        return running + jnp.stack([lax.optimization_barrier(jnp.sum(weights * delta_x, axis=-2)), lax.optimization_barrier(jnp.sum(weights * delta_y, axis=-2)), lax.optimization_barrier(jnp.sum(weights * delta_z, axis=-2))], axis=0)
    return lax.fori_loop(jnp.int32(0), jnp.int32(27), add_offset, jnp.zeros(targets.shape, jnp.float32))

def pull_grid(field):
    padded = jnp.pad(field, ((0, 0), (1, 1), (1, 1), (1, 1), (0, 0)), mode='wrap')

    def one_plane(plane_index):
        window = lax.dynamic_slice_in_dim(padded, plane_index, 3, axis=1)
        targets = lax.dynamic_slice_in_dim(field[:3], plane_index, 1, axis=1)
        return pull_block(window, targets)[:, 0]
    planes = lax.map(one_plane, jnp.arange(field.shape[1], dtype=jnp.int32))
    return jnp.moveaxis(planes, 0, 1)

def reference(halo_position, halo_velocity, halo_mass, cell_counts):
    occupied = lax.broadcasted_iota(jnp.int32, halo_mass.shape, 3) < cell_counts[..., None]
    held_mass = jnp.where(occupied, halo_mass, 0.0)
    first_pull = pull_grid(jnp.concatenate([halo_position, held_mass[None]], axis=0))
    drifted = halo_position + halo_velocity + 0.5 * first_pull
    second_pull = pull_grid(jnp.concatenate([drifted, held_mass[None]], axis=0))
    predicted = halo_position + halo_velocity + first_pull / 3.0 + second_pull / 6.0
    return jnp.where(occupied[None], predicted, 0.0)
```

```python
import functools
import itertools

import jax
import jax.numpy as jnp
import numpy as np
from jax import lax
from jax.experimental import pallas as pl
from jax.experimental.pallas import tpu as pltpu
from jax.sharding import PartitionSpec as P

soft_sq = 0.01
cut_sq = 0.64
scale = 1.25
soft = soft_sq * scale * scale
top = 1.0 + soft
gain = scale**3 / scale
far = 8.0
K = 48


def extended_2(cells, sides, width):
    for axis, dim in sides:
        count = lax.axis_size(axis)
        head = lax.slice_in_dim(cells, 0, width, axis=dim)
        tail = lax.slice_in_dim(cells, cells.shape[dim] - width, cells.shape[dim], axis=dim)
        cells = jnp.concatenate(
            [
                lax.ppermute(tail, axis, [(i, (i + 1) % count) for i in range(count)]),
                cells,
                lax.ppermute(head, axis, [((i + 1) % count, i) for i in range(count)]),
            ],
            axis=dim,
        )
    return cells


def parts_of(value):
    first = value.astype(jnp.bfloat16).astype(jnp.float32)
    rest = value - first
    second = rest.astype(jnp.bfloat16).astype(jnp.float32)
    third = (rest - second).astype(jnp.bfloat16).astype(jnp.float32)
    return first, second, third


def shift_tables():
    shifts = np.array(list(itertools.product((-1, 0, 1), repeat=3)), np.float32)
    offs = np.zeros((3, 32, 1), np.float32)
    offs[:, :27, 0] = scale * shifts.T
    offs = np.broadcast_to(offs, (3, 32, 128))
    rows = np.zeros((32, 16, 1), np.float32)
    for c in range(3):
        rows[:27, 3 + 3 * c : 6 + 3 * c, 0] = 2 * scale * shifts[:, c, None]
    return jnp.asarray(offs), jnp.asarray(np.broadcast_to(rows, (32, 16, 128)))


def pull_kernel(dims, src, offs, rows, out, a_scr, r_scr, t_scr, v_scr, row_scr, m_scr):
    dx, dy, dz = dims
    ey, ez = dy + 2, dz + 2
    cells = (dx + 2) * ey * ez
    ones = jnp.ones((8, 128), jnp.float32)
    zeros = jnp.zeros((8, 128), jnp.float32)
    v_scr[...] = rows[...]

    @pl.loop(0, cells // 8)
    def _(group):
        base = pl.multiple_of(group * 8, 8)
        mass = src[3, pl.ds(base, 8), :]
        a = [(src[c, pl.ds(base, 8), :] - 0.5) * scale for c in range(3)]
        a = [jnp.where(mass > 0.0, v, 0.0) for v in a]
        split = [parts_of(v) for v in a]
        norm = parts_of(a[0] * a[0] + a[1] * a[1] + a[2] * a[2])
        left = []
        for p in split:
            left += [p[0], p[0], p[1], p[0], p[2], p[1]]
        left += list(norm) + [zeros] * 11 + [ones] * 3
        for p in split:
            left += list(p)
        left += [zeros] * (K - len(left))
        for k, v in enumerate(left):
            row_scr[:, k, :] = v
        right = []
        for c in range(3):
            p = parts_of(a[c] * -2.0)
            right += [p[0], p[1], p[0], p[2], p[0], p[1]]
        right += [ones] * 3 + [zeros] * 11
        mm = [parts_of(mass * v) for v in a] + [parts_of(mass)]
        order = list(mm[0]) + list(mm[1]) + [zeros] * 2 + list(mm[2]) + list(mm[3]) + [zeros] * 2
        for k, v in enumerate(order):
            m_scr[:, k, :] = v
        for j in range(8):
            a_scr[base + j] = row_scr[j].T.astype(jnp.bfloat16)
            r = m_scr[j].astype(jnp.bfloat16)
            r_scr[base + j] = jnp.concatenate([r, r], axis=1)
        for k, v in enumerate(right):
            row_scr[:, k, :] = v
        for j in range(8):
            t_scr[base + j] = row_scr[j, :32].astype(jnp.bfloat16)

    @pl.loop(0, dx * dy * dz)
    def _(i):
        x = i // (dy * dz)
        y = i // dz % dy
        z = i % dz
        me = ((x + 1) * ey + y + 1) * ez + z + 1
        held = src[3, pl.ds(me, 1), :] > 0.0
        t = [jnp.where(held, (src[c, pl.ds(me, 1), :] - 0.5) * scale, 0.0) for c in range(3)]
        norm = soft
        for c in range(3):
            d = t[c] - offs[c]
            norm = norm + d * d
        for k, v in enumerate(parts_of(norm)):
            v_scr[:, k, :] = v
        fixed = t_scr[me]
        reach = jnp.max(jnp.maximum(jnp.maximum(jnp.abs(t[0]), jnp.abs(t[1])), jnp.abs(t[2])))

        @pl.when(reach <= far)
        def _():
            def plane(sx, carry):
                acc, lean_x, lean_y, lean_z = carry
                total = jnp.zeros((8, 128), jnp.float32)
                for sy in range(3):
                    for sz in range(3):
                        other = ((x + sx) * ey + y + sy) * ez + z + sz
                        right = jnp.concatenate(
                            [fixed, v_scr[sx * 9 + sy * 3 + sz].astype(jnp.bfloat16)], axis=0
                        )
                        v = jnp.dot(a_scr[other], right, preferred_element_type=jnp.float32)
                        r = lax.rsqrt(v)
                        g = r * jnp.maximum(top - v, 0.0)
                        w = g * g * r
                        hi = w.astype(jnp.bfloat16)
                        lo = (w - hi.astype(jnp.float32)).astype(jnp.bfloat16)
                        f = jnp.dot(
                            r_scr[other],
                            jnp.concatenate([hi, lo], axis=0),
                            preferred_element_type=jnp.float32,
                        )
                        acc = acc + f
                        m = f[8:]
                        total = total + m
                        if sy != 1:
                            lean_y = lean_y + m * float(sy - 1)
                        if sz != 1:
                            lean_z = lean_z + m * float(sz - 1)
                lean_x = lean_x + total * (sx - 1).astype(jnp.float32)
                return acc, lean_x, lean_y, lean_z

            acc, *leans = lax.fori_loop(
                0, 3, plane, (jnp.zeros((16, 128), jnp.float32), zeros, zeros, zeros)
            )

            def three(v, k):
                return v[k : k + 1] + v[k + 1 : k + 2] + v[k + 2 : k + 3]

            m = three(acc, 11)
            for c, k in enumerate((0, 3, 8)):
                out[c, pl.ds(i, 1), :] = gain * (three(acc, k) + scale * three(leans[c], 3) - t[c] * m)

        @pl.when(reach > far)
        def _():
            def one(code, carry):
                sx, sy, sz = code // 9, code // 3 % 3, code % 3
                other = ((x + sx) * ey + y + sy) * ez + z + sz
                for k in range(4):
                    m_scr[0, k : k + 1, :] = src[k, pl.ds(other, 1), :]
                cols = m_scr[0, :8].T
                deltas = []
                q = 0.0
                for c, s in enumerate((sx, sy, sz)):
                    d = cols[:, c : c + 1] + (s - 1).astype(jnp.float32) - src[c, pl.ds(me, 1), :]
                    deltas.append(d)
                    q = q + d * d
                r = lax.rsqrt(q + soft_sq)
                taper = jnp.maximum(1.0 - q * (1.0 / cut_sq), 0.0)
                w = cols[:, 3:4] * (r * r * r) * (taper * taper)
                return tuple(
                    v + jnp.sum(w * d, axis=0, keepdims=True) for v, d in zip(carry, deltas)
                )

            zero = jnp.zeros((1, 128), jnp.float32)
            pulls = lax.fori_loop(0, 27, one, (zero, zero, zero))
            for c in range(3):
                out[c, pl.ds(i, 1), :] = pulls[c]


def pull_field(extended):
    _, ex, ey, ez, slots = extended.shape
    dims = (ex - 2, ey - 2, ez - 2)
    cells = ex * ey * ez
    offs, rows = shift_tables()
    own = dims[0] * dims[1] * dims[2]
    pulls = pl.pallas_call(
        functools.partial(pull_kernel, dims),
        out_shape=jax.ShapeDtypeStruct((3, own, slots), jnp.float32),
        in_specs=[pl.BlockSpec(memory_space=pltpu.VMEM)] * 3,
        out_specs=pl.BlockSpec(memory_space=pltpu.VMEM),
        scratch_shapes=[
            pltpu.VMEM((cells, slots, K), jnp.bfloat16),
            pltpu.VMEM((cells, 16, 2 * slots), jnp.bfloat16),
            pltpu.VMEM((cells, 32, slots), jnp.bfloat16),
            pltpu.VMEM((32, 16, slots), jnp.float32),
            pltpu.VMEM((8, K, slots), jnp.float32),
            pltpu.VMEM((8, 16, slots), jnp.float32),
        ],
        compiler_params=pltpu.CompilerParams(vmem_limit_bytes=48 * 2**20),
        name="pulls",
    )(extended.reshape(4, cells, slots), offs, rows)
    return pulls.reshape((3,) + dims + (slots,))


def body(halo_position, halo_velocity, halo_mass, cell_counts):
    occupied = lax.broadcasted_iota(jnp.int32, halo_mass.shape, 3) < cell_counts[..., None]
    held_mass = jnp.where(occupied, halo_mass, 0.0)
    outgoing = jnp.concatenate([halo_position, held_mass[None]], axis=0)
    mass_rim = None
    first_pull = None
    second_pull = None
    for round_index in range(2):
        widened = extended_2(outgoing, (("gx", 1),), 1)
        widened = extended_2(widened, (("gy", 2),), 1)
        widened = extended_2(widened, (("gz", 3),), 1)
        if round_index == 0:
            mass_rim = widened[3:4]
            first_pull = pull_field(widened)
            outgoing = halo_position + halo_velocity + 0.5 * first_pull
        else:
            second_pull = pull_field(jnp.concatenate([widened, mass_rim], axis=0))
    predicted = halo_position + halo_velocity + first_pull / 3.0 + second_pull / 6.0
    return jnp.where(occupied[None], predicted, 0.0)


def solution(mesh):
    return jax.shard_map(
        body,
        mesh=mesh,
        in_specs=(
            P(None, "gx", "gy", "gz", None),
            P(None, "gx", "gy", "gz", None),
            P("gx", "gy", "gz", None),
            P("gx", "gy", "gz"),
        ),
        out_specs=P(None, "gx", "gy", "gz", None),
        check_vma=False,
    )
```

```python
import functools
import itertools

import jax
import jax.numpy as jnp
import numpy as np
from jax import lax
from jax.experimental import pallas as pl
from jax.experimental.pallas import tpu as pltpu
from jax.sharding import PartitionSpec as P

soft_sq = 0.01
cut_sq = 0.64
scale = 1.25
soft = soft_sq * scale * scale
top = 1.0 + soft
gain = scale**3 / scale
far = 8.0
K = 48


def extended_2(cells, sides, width):
    for axis, dim in sides:
        count = lax.axis_size(axis)
        head = lax.slice_in_dim(cells, 0, width, axis=dim)
        tail = lax.slice_in_dim(cells, cells.shape[dim] - width, cells.shape[dim], axis=dim)
        cells = jnp.concatenate(
            [
                lax.ppermute(tail, axis, [(i, (i + 1) % count) for i in range(count)]),
                cells,
                lax.ppermute(head, axis, [((i + 1) % count, i) for i in range(count)]),
            ],
            axis=dim,
        )
    return cells


def parts_of(value):
    first = value.astype(jnp.bfloat16).astype(jnp.float32)
    rest = value - first
    second = rest.astype(jnp.bfloat16).astype(jnp.float32)
    third = (rest - second).astype(jnp.bfloat16).astype(jnp.float32)
    return first, second, third


def shift_tables():
    shifts = np.array(list(itertools.product((-1, 0, 1), repeat=3)), np.float32)
    offs = np.zeros((3, 32, 1), np.float32)
    offs[:, :27, 0] = scale * shifts.T
    offs = np.broadcast_to(offs, (3, 32, 128))
    rows = np.zeros((32, 16, 1), np.float32)
    for c in range(3):
        rows[:27, 3 + 3 * c : 6 + 3 * c, 0] = 2 * scale * shifts[:, c, None]
    return jnp.asarray(offs), jnp.asarray(np.broadcast_to(rows, (32, 16, 128)))


def pull_kernel(dims, width, src, offs, rows, out, a_scr, r_scr, t_scr, v_scr, row_scr, m_scr, w_scr):
    dx, dy, dz = dims
    ey, ez = dy + 2, dz + 2
    cells = (dx + 2) * ey * ez
    ones = jnp.ones((8, 128), jnp.float32)
    zeros = jnp.zeros((8, 128), jnp.float32)
    for n in range(v_scr.shape[0]):
        v_scr[n] = rows[...]
    row_scr[...] = jnp.zeros(row_scr.shape, jnp.float32)
    m_scr[...] = jnp.zeros(m_scr.shape, jnp.float32)
    w_scr[...] = jnp.zeros(w_scr.shape, jnp.float32)
    for k in range(3):
        row_scr[:, 32 + k, :] = ones
        w_scr[:, 18 + k, :] = ones

    @pl.loop(0, cells // 8, unroll=2)
    def _(group):
        base = pl.multiple_of(group * 8, 8)
        mass = src[3, pl.ds(base, 8), :]
        a = [(src[c, pl.ds(base, 8), :] - 0.5) * scale for c in range(3)]
        a = [jnp.where(mass > 0.0, v, 0.0) for v in a]
        split = [parts_of(v) for v in a]
        norm = parts_of(a[0] * a[0] + a[1] * a[1] + a[2] * a[2])
        left = []
        for p in split:
            left += [p[0], p[0], p[1], p[0], p[2], p[1]]
        left += list(norm) + [None] * 14
        for p in split:
            left += list(p)
        for k, v in enumerate(left):
            if v is not None:
                row_scr[:, k, :] = v
        right = []
        for c in range(3):
            p = parts_of(a[c] * -2.0)
            right += [p[0], p[1], p[0], p[2], p[0], p[1]]
        mm = [parts_of(mass * v) for v in a] + [parts_of(mass)]
        order = list(mm[0]) + list(mm[1]) + [None] * 2 + list(mm[2]) + list(mm[3])
        for k, v in enumerate(order):
            if v is not None:
                m_scr[:, k, :] = v
        for j in range(8):
            a_scr[base + j] = row_scr[j].T.astype(jnp.bfloat16)
            r = m_scr[j].astype(jnp.bfloat16)
            r_scr[base + j] = jnp.concatenate([r, r], axis=1)
        for k, v in enumerate(right):
            w_scr[:, k, :] = v
        for j in range(8):
            t_scr[base + j] = w_scr[j].astype(jnp.bfloat16)

    def near(i, v_scr):
        x = i // (dy * dz)
        y = i // dz % dy
        z = i % dz
        me = ((x + 1) * ey + y + 1) * ez + z + 1
        held = src[3, pl.ds(me, 1), :] > 0.0
        t = [jnp.where(held, (src[c, pl.ds(me, 1), :] - 0.5) * scale, 0.0) for c in range(3)]
        norm = soft
        for c in range(3):
            d = t[c] - offs[c]
            norm = norm + d * d
        for k, v in enumerate(parts_of(norm)):
            v_scr[:, k, :] = v
        fixed = t_scr[me]
        reach = jnp.max(jnp.maximum(jnp.maximum(jnp.abs(t[0]), jnp.abs(t[1])), jnp.abs(t[2])))

        acc = jnp.zeros((16, 128), jnp.float32)
        leans = [zeros, zeros, zeros]
        for code, shift in enumerate(itertools.product(range(3), repeat=3)):
            other = ((x + shift[0]) * ey + y + shift[1]) * ez + z + shift[2]
            right = jnp.concatenate([fixed, v_scr[code].astype(jnp.bfloat16)], axis=0)
            v = jnp.dot(a_scr[other], right, preferred_element_type=jnp.float32)
            r = lax.rsqrt(v)
            g = r * jnp.maximum(top - v, 0.0)
            w = g * g * r
            hi = w.astype(jnp.bfloat16)
            lo = (w - hi.astype(jnp.float32)).astype(jnp.bfloat16)
            f = jnp.dot(
                r_scr[other],
                jnp.concatenate([hi, lo], axis=0),
                preferred_element_type=jnp.float32,
            )
            acc = acc + f
            for c in range(3):
                if shift[c] != 1:
                    leans[c] = leans[c] + f[8:] * float(shift[c] - 1)

        def three(v, k):
            return v[k : k + 1] + v[k + 1 : k + 2] + v[k + 2 : k + 3]

        m = three(acc, 11)
        for c, k in enumerate((0, 3, 8)):
            out[c, pl.ds(i, 1), :] = gain * (three(acc, k) + scale * three(leans[c], 3) - t[c] * m)
        return reach

    def afar(i, reach):
        x = i // (dy * dz)
        y = i // dz % dy
        z = i % dz
        me = ((x + 1) * ey + y + 1) * ez + z + 1

        @pl.when(reach > far)
        def _():
            def one(code, carry):
                sx, sy, sz = code // 9, code // 3 % 3, code % 3
                other = ((x + sx) * ey + y + sy) * ez + z + sz
                for k in range(4):
                    w_scr[0, k : k + 1, :] = src[k, pl.ds(other, 1), :]
                cols = w_scr[0, :8].T
                deltas = []
                q = 0.0
                for c, s in enumerate((sx, sy, sz)):
                    d = cols[:, c : c + 1] + (s - 1).astype(jnp.float32) - src[c, pl.ds(me, 1), :]
                    deltas.append(d)
                    q = q + d * d
                r = lax.rsqrt(q + soft_sq)
                taper = jnp.maximum(1.0 - q * (1.0 / cut_sq), 0.0)
                w = cols[:, 3:4] * (r * r * r) * (taper * taper)
                return tuple(
                    v + jnp.sum(w * d, axis=0, keepdims=True) for v, d in zip(carry, deltas)
                )

            zero = jnp.zeros((1, 128), jnp.float32)
            pulls = lax.fori_loop(0, 27, one, (zero, zero, zero))
            for c in range(3):
                out[c, pl.ds(i, 1), :] = pulls[c]

    @pl.loop(0, dx * dy * dz // width)
    def _(step):
        reaches = [near(step * width + n, v_scr.at[n]) for n in range(width)]
        for n in range(width):
            afar(step * width + n, reaches[n])


def pull_field(extended):
    _, ex, ey, ez, slots = extended.shape
    dims = (ex - 2, ey - 2, ez - 2)
    cells = ex * ey * ez
    offs, rows = shift_tables()
    own = dims[0] * dims[1] * dims[2]
    width = 4 if own % 4 == 0 else 1
    pulls = pl.pallas_call(
        functools.partial(pull_kernel, dims, width),
        out_shape=jax.ShapeDtypeStruct((3, own, slots), jnp.float32),
        in_specs=[pl.BlockSpec(memory_space=pltpu.VMEM)] * 3,
        out_specs=pl.BlockSpec(memory_space=pltpu.VMEM),
        scratch_shapes=[
            pltpu.VMEM((cells, slots, K), jnp.bfloat16),
            pltpu.VMEM((cells, 16, 2 * slots), jnp.bfloat16),
            pltpu.VMEM((cells, 32, slots), jnp.bfloat16),
            pltpu.VMEM((width, 32, 16, slots), jnp.float32),
            pltpu.VMEM((8, K, slots), jnp.float32),
            pltpu.VMEM((8, 16, slots), jnp.float32),
            pltpu.VMEM((8, 32, slots), jnp.float32),
        ],
        compiler_params=pltpu.CompilerParams(vmem_limit_bytes=48 * 2**20),
        name="pulls",
    )(extended.reshape(4, cells, slots), offs, rows)
    return pulls.reshape((3,) + dims + (slots,))


def body(halo_position, halo_velocity, halo_mass, cell_counts):
    occupied = lax.broadcasted_iota(jnp.int32, halo_mass.shape, 3) < cell_counts[..., None]
    held_mass = jnp.where(occupied, halo_mass, 0.0)
    outgoing = jnp.concatenate([halo_position, held_mass[None]], axis=0)
    mass_rim = None
    first_pull = None
    second_pull = None
    for round_index in range(2):
        widened = extended_2(outgoing, (("gx", 1),), 1)
        widened = extended_2(widened, (("gy", 2),), 1)
        widened = extended_2(widened, (("gz", 3),), 1)
        if round_index == 0:
            mass_rim = widened[3:4]
            first_pull = pull_field(widened)
            outgoing = halo_position + halo_velocity + 0.5 * first_pull
        else:
            second_pull = pull_field(jnp.concatenate([widened, mass_rim], axis=0))
    predicted = halo_position + halo_velocity + first_pull / 3.0 + second_pull / 6.0
    return jnp.where(occupied[None], predicted, 0.0)


def solution(mesh):
    return jax.shard_map(
        body,
        mesh=mesh,
        in_specs=(
            P(None, "gx", "gy", "gz", None),
            P(None, "gx", "gy", "gz", None),
            P("gx", "gy", "gz", None),
            P("gx", "gy", "gz"),
        ),
        out_specs=P(None, "gx", "gy", "gz", None),
        check_vma=False,
    )
```
